32 devices in a mesh: section: 4 (over y, core), dp: 2 (over x), tensor: 4 (over z).
Axes of the slice: x: 2, y: 2, z: 4, core: 2. Of those that a mesh axis runs over, the one named last changes fastest.
Arguments:
- shadow_weight_copy: bfloat16 [4, 4096, 4096], P('section', None, 'tensor'), may hold values from -6 to 6
- newest_weight_version: bfloat16 [4, 4096, 4096], P('section', 'dp', 'tensor'), may hold values from -6 to 6
- momentum: bfloat16 [4, 4096, 4096], P('section', 'dp', 'tensor'), may hold values from -3 to 3
- pending_section_input: bfloat16 [2, 4, 64, 4096], P('dp', 'section', None, 'tensor'), may hold values from -16 to 16
- incoming_micro_input: bfloat16 [2, 3, 64, 4096], P('dp', None, None, 'tensor'), may hold values from -16 to 16
- pending_output_gradient: bfloat16 [2, 4, 64, 4096], P('dp', 'section', None, 'tensor'), may hold values from -16 to 16
- loss_gradient_rows: bfloat16 [2, 3, 64, 4096], P('dp', None, None, 'tensor'), may hold values from -16 to 16
- stashed: bfloat16 [2, 4, 4, 64, 4096], P('dp', 'section', None, None, 'tensor'), may hold values from -16 to 16
Outputs:
- forward_out: bfloat16 [2, 4, 4, 64, 4096], P('dp', 'section', None, None, 'tensor')
- backward_out: bfloat16 [2, 4, 4, 64, 4096], P('dp', 'section', None, None, 'tensor')
- w_next: bfloat16 [4, 4096, 4096], P('section', 'dp', 'tensor')
- m_next: bfloat16 [4, 4096, 4096], P('section', 'dp', 'tensor')
The draws below stay inside these ranges and needn't reach their ends.
All inputs are finite; a program needn't handle non-finite values.
Results may differ from the reference program's by a relative error of at most 0.025.
Values may be sent and summed in bfloat16 or wider, within the bound.
A program may use at most 128 MiB of HBM per device.

```python
import math
import jax
import jax.numpy as jnp
from jax import lax

D = 4096
ROWS = 64
TICKS = 4
SECTIONS = 4
REPLICAS = 2
N_TENSOR = 4


def feature_field(key, dimensions):
    extent = dimensions[-1]
    random_part = jax.random.normal(jax.random.fold_in(key, 1), dimensions, jnp.float32)
    growth = jnp.exp(jnp.log(3.0) * jnp.arange(extent, dtype=jnp.float32) / (extent - 1))
    result_field = random_part * growth / jnp.sqrt(jnp.mean(growth * growth))
    return jnp.clip(result_field, -16.0, 16.0).astype(jnp.bfloat16)


def draw_pending_section_input(key, part):
    return feature_field(jax.random.fold_in(key, 101), (REPLICAS, SECTIONS, ROWS, D))


def draw_incoming_micro_input(key, part):
    return feature_field(jax.random.fold_in(key, 102), (REPLICAS, TICKS - 1, ROWS, D))


def draw_pending_output_gradient(key, part):
    return feature_field(jax.random.fold_in(key, 103), (REPLICAS, SECTIONS, ROWS, D))


def draw_loss_gradient_rows(key, part):
    return feature_field(jax.random.fold_in(key, 104), (REPLICAS, TICKS - 1, ROWS, D))


def draw_stashed(key, part):
    return feature_field(jax.random.fold_in(key, 105), (REPLICAS, SECTIONS, TICKS, ROWS, D))


def block_scale(rng, dims, cuts, least, largest):
    gain, own = 1.0, jax.random.fold_in(rng, 6)
    for position, shards_of in cuts:
        steps = jnp.exp(jax.random.uniform(jax.random.fold_in(own, position), (shards_of,), jnp.float32, least / len(cuts), largest / len(cuts)))
        gain = gain * jnp.repeat(steps, dims[position] // shards_of).reshape([-1 if axis == position else 1 for axis in range(len(dims))])
    return gain


def scatter_about(own_key, shape, spread, bound, split=(), kind=jnp.bfloat16):
    values = spread * jax.random.normal(own_key, shape, jnp.float32)
    if split:
        values = values * block_scale(own_key, shape, split, -0.22, 0.18)
    return jnp.clip(values, -bound, bound).astype(kind)


def setup_inputs(seed: int = 0) -> dict:
    streams_of = jax.random.split(jax.random.key(seed), 9)
    shadow_weight_copy = scatter_about(streams_of[0], (SECTIONS, D, D), 1.0, 6.0, ((0, 4), (2, 4)))
    newest_weight_version = scatter_about(streams_of[1], (SECTIONS, D, D), 1.0, 6.0, ((0, 4), (1, 2), (2, 4)))
    momentum = scatter_about(streams_of[2], (SECTIONS, D, D), 0.5, 3.0, ((0, 4), (1, 2), (2, 4)))
    pending_section_input = draw_pending_section_input(jax.random.fold_in(streams_of[8], 71), 0)
    incoming_micro_input = draw_incoming_micro_input(jax.random.fold_in(streams_of[8], 71), 0)
    pending_output_gradient = draw_pending_output_gradient(jax.random.fold_in(streams_of[8], 71), 0)
    loss_gradient_rows = draw_loss_gradient_rows(jax.random.fold_in(streams_of[8], 71), 0)
    stashed = draw_stashed(jax.random.fold_in(streams_of[8], 71), 0)
    return {"shadow_weight_copy": shadow_weight_copy, "newest_weight_version": newest_weight_version, "momentum": momentum, "pending_section_input": pending_section_input, "incoming_micro_input": incoming_micro_input, "pending_output_gradient": pending_output_gradient, "loss_gradient_rows": loss_gradient_rows, "stashed": stashed}


EPSILON = 1e-06
MOMENTUM_RATE = 0.9
LEARNING_RATE = 0.05

def normalized(values):
    factor = lax.rsqrt(lax.optimization_barrier(jnp.mean(values * values, axis=-1, keepdims=True)) + EPSILON)
    return (values * factor, factor)

def rounded(values):
    return lax.optimization_barrier(values.astype(jnp.bfloat16)).astype(jnp.float32)

def section_tick(operands):
    current_input, kept_in, grad_in, weight = operands
    extent = weight.shape[0]
    root_width = math.sqrt(extent)
    weight_wide = weight.astype(jnp.float32)
    x_wide = current_input.astype(jnp.float32)
    x_hat, unused = normalized(x_wide)
    branch = jnp.einsum('prd,de->pre', rounded(x_hat), weight_wide) / root_width
    section_out = (x_wide + branch).astype(jnp.bfloat16)
    kept_hat, kept_factor = normalized(kept_in.astype(jnp.float32))
    grad_wide = grad_in.astype(jnp.float32)
    replicas = grad_in.shape[0]
    row_count = grad_in.shape[1]
    shard_cols = extent // N_TENSOR
    grad_pieces = grad_wide.reshape(replicas, row_count, N_TENSOR, shard_cols)
    weight_pieces = weight_wide.reshape(extent, N_TENSOR, shard_cols)
    partial_value = jnp.einsum('prje,dje->pjrd', grad_pieces, weight_pieces) / root_width
    branch_grad = lax.optimization_barrier(jnp.sum(rounded(partial_value), axis=1))
    inner_dot = lax.optimization_barrier(jnp.mean(branch_grad * kept_hat, axis=-1, keepdims=True))
    input_grad = (grad_wide + (branch_grad - kept_hat * inner_dot) * kept_factor).astype(jnp.bfloat16)
    return (section_out, input_grad, kept_hat.astype(jnp.bfloat16))

def section_update(operands):
    kept_rows, grad_rows, latest, moment = operands
    extent = latest.shape[0]
    replica_terms = jnp.einsum('pkrd,pkre->pde', kept_rows.astype(jnp.float32), grad_rows.astype(jnp.float32)) / math.sqrt(extent)
    summed = lax.optimization_barrier(jnp.sum(rounded(replica_terms), axis=0))
    velocity = MOMENTUM_RATE * moment.astype(jnp.float32) + summed
    new_weight = (latest.astype(jnp.float32) - LEARNING_RATE * velocity).astype(jnp.bfloat16)
    return (new_weight, velocity.astype(jnp.bfloat16))

def reference(shadow_weight_copy, newest_weight_version, momentum, pending_section_input, incoming_micro_input, pending_output_gradient, loss_gradient_rows, stashed):
    tick_count = stashed.shape[2]
    current_input = pending_section_input
    current_gradient = pending_output_gradient
    forward_list = []
    backward_list = []
    kept_list = []
    grad_list = []
    for tick_index in range(tick_count):
        if tick_index > 0:
            current_input = jnp.concatenate([incoming_micro_input[:, tick_index - 1][:, None], forward_list[-1][:, :-1]], axis=1)
            current_gradient = jnp.concatenate([backward_list[-1][:, 1:], loss_gradient_rows[:, tick_index - 1][:, None]], axis=1)
        operands = (jnp.moveaxis(current_input, 1, 0), jnp.moveaxis(stashed[:, :, tick_index], 1, 0), jnp.moveaxis(current_gradient, 1, 0), shadow_weight_copy)
        section_out, input_grad, kept_norm = lax.map(section_tick, operands)
        forward_list.append(jnp.moveaxis(section_out, 0, 1))
        backward_list.append(jnp.moveaxis(input_grad, 0, 1))
        kept_list.append(jnp.moveaxis(kept_norm, 0, 1))
        grad_list.append(current_gradient)
    forward_out = jnp.stack(forward_list, axis=2)
    backward_out = jnp.stack(backward_list, axis=2)
    kept_all = jnp.stack(kept_list, axis=2)
    grad_all = jnp.stack(grad_list, axis=2)
    w_next, m_next = lax.map(section_update, (jnp.moveaxis(kept_all, 1, 0), jnp.moveaxis(grad_all, 1, 0), newest_weight_version, momentum))
    return (forward_out, backward_out, w_next, m_next)
```

```python
import functools
import math

import jax
import jax.numpy as jnp
from jax import lax
from jax.experimental import pallas as pl
from jax.experimental.pallas import tpu as pltpu
from jax.sharding import PartitionSpec as P

EPSILON = 1e-06
MOMENTUM_RATE = 0.9
LEARNING_RATE = 0.05
MESH = pl.DeviceIdType.MESH
LANES = 128


def remote(src, dst, send_sem, recv_sem, target):
    return pltpu.make_async_remote_copy(
        src_ref=src,
        dst_ref=dst,
        send_sem=send_sem,
        recv_sem=recv_sem,
        device_id=target,
        device_id_type=MESH,
    )


def rowsum(values):
    return jnp.sum(values, axis=-1, keepdims=True)


def window_kernel(
    n, dp, sections,
    w_hbm, x0_hbm, inc_hbm, g0_hbm, loss_hbm, stash_hbm,
    fwd, bwd, st_all, sg_all,
    w, xg, st, gbuf, prod, acc, ssq, stw, ksc, sgs,
    rs_s, rs_r, inm, inb,
    lsem, x_ss, x_rs, st_ss, st_rs, rs_ss, rs_rs,
    f_ss, f_rs, b_ss, b_rs, in_ss, in_rs,
    dst_ss, dst_rs, dsg_ss, dsg_rs, own_sem,
):
    j = lax.axis_index("tensor")
    d = lax.axis_index("dp")
    s = lax.axis_index("section")
    ticks, _, rows, cols = xg.shape
    extent = n * cols
    root = math.sqrt(extent)
    nb = n // dp
    first, last = s == 0, s == sections - 1

    def both(a, b):
        return jnp.logical_and(a, b)

    w_copy = pltpu.make_async_copy(w_hbm, w, lsem.at[0])
    st_copy = pltpu.make_async_copy(stash_hbm, st.at[:, j], lsem.at[1])
    x_copy = pltpu.make_async_copy(x0_hbm, xg.at[0, j], lsem.at[2])
    g_copy = pltpu.make_async_copy(g0_hbm, gbuf.at[0], lsem.at[3])
    inc_copy = pltpu.make_async_copy(inc_hbm, xg.at[pl.ds(1, ticks - 1), j], lsem.at[4])
    loss_copy = pltpu.make_async_copy(loss_hbm, gbuf.at[pl.ds(1, ticks - 1)], lsem.at[5])
    st_copy.start()
    x_copy.start()
    g_copy.start()
    pl.when(first)(lambda: inc_copy.start())
    pl.when(last)(lambda: loss_copy.start())
    w_copy.start()

    barrier = pltpu.get_barrier_semaphore()
    for q in range(1, n):
        pl.semaphore_signal(
            barrier, inc=1, device_id={"tensor": lax.rem(j + q, n)}, device_id_type=MESH
        )
    for q in range(1, dp):
        pl.semaphore_signal(
            barrier, inc=1, device_id={"dp": lax.rem(d + q, dp)}, device_id_type=MESH
        )

    @pl.when(s > 0)
    def _():
        pl.semaphore_signal(barrier, inc=1, device_id={"section": s - 1}, device_id_type=MESH)

    @pl.when(s < sections - 1)
    def _():
        pl.semaphore_signal(barrier, inc=1, device_id={"section": s + 1}, device_id_type=MESH)

    peers = n - 1 + dp - 1 + jnp.where(s > 0, 1, 0) + jnp.where(s < sections - 1, 1, 0)
    pl.semaphore_wait(barrier, peers)
    st_copy.wait()
    x_copy.wait()
    g_copy.wait()
    pl.when(first)(lambda: inc_copy.wait())
    pl.when(last)(lambda: loss_copy.wait())

    def line_copy(buf, ss, rs, t, side, k, block):
        return remote(
            buf.at[t, block], buf.at[t, block], ss.at[t, side, k], rs.at[t, side, k],
            {"tensor": j + 1 if side == 0 else j - 1},
        )

    def send_ok(side, k):
        if side == 0:
            return both(j < n - 1, j - k >= 0)
        return both(j > 0, j + k <= n - 1)

    def line_send(buf, ss, rs, t, side, k, extra=None):
        if k > n - 2:
            return
        ok = send_ok(side, k)
        ok = ok if extra is None else both(ok, extra)

        @pl.when(ok)
        def _():
            line_copy(buf, ss, rs, t, side, k, j - k if side == 0 else j + k).start()

    def line_sent(buf, ss, rs, t, side, k):
        @pl.when(send_ok(side, k))
        def _():
            line_copy(buf, ss, rs, t, side, k, j - k if side == 0 else j + k).wait_send()

    def arrives(side, k):
        return j - 1 - k >= 0 if side == 0 else j + 1 + k <= n - 1

    def line_recv(buf, ss, rs, t, side, k, extra=None):
        ok = arrives(side, k)
        ok = ok if extra is None else both(ok, extra)
        block = j - 1 - k if side == 0 else j + 1 + k

        @pl.when(ok)
        def _():
            remote(
                buf.at[t, block], buf.at[t, block], ss.at[t, side, k], rs.at[t, side, k],
                {"tensor": j - 1 if side == 0 else j + 1},
            ).wait_recv()

    xs = (xg, x_ss, x_rs)
    sts = (st, st_ss, st_rs)

    def dp_stash(t, q, i):
        peer = lax.rem(d + q, dp)
        return remote(
            st.at[t, peer * nb + i], st_all.at[i, d, t],
            dst_ss.at[t, q - 1, i], dst_rs.at[t, q - 1, i], {"dp": peer},
        )

    def dp_stash_in(t, q, i):
        peer = lax.rem(d + dp - q, dp)
        return remote(
            st.at[t, i], st_all.at[i, peer, t],
            dst_ss.at[t, q - 1, i], dst_rs.at[t, q - 1, i], {"dp": peer},
        )

    def dp_grad(t, q):
        peer = lax.rem(d + q, dp)
        return remote(
            sgs.at[t], sg_all.at[d, t], dsg_ss.at[t, q - 1], dsg_rs.at[t, q - 1], {"dp": peer}
        )

    def dp_grad_in(t, q):
        peer = lax.rem(d + dp - q, dp)
        return remote(
            sgs.at[t], sg_all.at[peer, t], dsg_ss.at[t, q - 1], dsg_rs.at[t, q - 1], {"dp": peer}
        )

    def own_stash(t, i):
        return pltpu.make_async_copy(st.at[t, d * nb + i], st_all.at[i, d, t], own_sem.at[t, i])

    def own_grad_copy(t):
        return pltpu.make_async_copy(sgs.at[t], sg_all.at[d, t], own_sem.at[t, nb])

    def stash_finish(t):
        for q in range(1, dp):
            for i in range(nb):
                dp_stash(t, q, i).start()
        for i in range(nb):
            own_stash(t, i).start()
        stw[...] = jnp.zeros_like(stw)

        def one(b, total):
            block = st[t, b]
            stw[...] += jnp.dot(block, w[b], preferred_element_type=jnp.float32)
            wide = block.astype(jnp.float32)
            return total + rowsum(wide * wide)

        total = lax.fori_loop(0, n, one, jnp.zeros((rows, 1), jnp.float32))
        ksc[...] = jnp.broadcast_to(lax.rsqrt(total / extent + EPSILON), ksc.shape)

    def rs_copy(t, side, k):
        return remote(
            rs_s.at[t, side, k], rs_r.at[t, side, k], rs_ss.at[t, side, k], rs_rs.at[t, side, k],
            {"tensor": j + 1 if side == 0 else j - 1},
        )

    def rs_in(t, side, k):
        return remote(
            rs_s.at[t, side, 0], rs_r.at[t, side, k], rs_ss.at[t, side, 0], rs_rs.at[t, side, k],
            {"tensor": j - 1 if side == 0 else j + 1},
        )

    def inner_copy(t, q):
        return remote(
            inm.at[t], inb.at[t, q - 1], in_ss.at[t, q - 1], in_rs.at[t, q - 1],
            {"tensor": lax.rem(j + q, n)},
        )

    def inner_in(t, q):
        return remote(
            inm.at[t], inb.at[t, q - 1], in_ss.at[t, q - 1], in_rs.at[t, q - 1],
            {"tensor": lax.rem(j + n - q, n)},
        )

    def fwd_copy(t):
        return remote(
            fwd.at[t], xg.at[t + 1, j], f_ss.at[t + 1], f_rs.at[t + 1], {"section": s + 1}
        )

    def bwd_copy(t):
        return remote(
            bwd.at[t], gbuf.at[t + 1], b_ss.at[t + 1], b_rs.at[t + 1], {"section": s - 1}
        )

    order = []
    for k in range((n + 1) // 2):
        order += [n - 1 - k] + ([k] if k != n - 1 - k else [])

    for side in range(2):
        line_send(*sts, 0, side, 0)
    for k in range(n - 1):
        for side in range(2):
            line_recv(*sts, 0, side, k)
            line_send(*sts, 0, side, k + 1)
    w_copy.wait()
    stash_finish(0)

    def tick(t, carry):
        more = t < ticks - 1

        @pl.when(both(t > 0, s > 0))
        def _():
            remote(
                fwd.at[t], xg.at[t, j], f_ss.at[t], f_rs.at[t], {"section": s - 1}
            ).wait_recv()

        for side in range(2):
            line_send(*xs, t, side, 0)

        @pl.when(both(t > 0, s < sections - 1))
        def _():
            remote(
                bwd.at[t], gbuf.at[t], b_ss.at[t], b_rs.at[t], {"section": s + 1}
            ).wait_recv()

        wide = gbuf[t].astype(jnp.float32)
        products = wide * stw[...]
        part = products[:, :LANES]
        for i in range(1, cols // LANES):
            part = part + products[:, i * LANES:(i + 1) * LANES]
        inm[t] = part
        sgs[t] = (wide * (ksc[:, :1] * (1.0 / root))).astype(jnp.bfloat16)
        for q in range(1, n):
            inner_copy(t, q).start()
        for q in range(1, dp):
            dp_grad(t, q).start()
        own_grad_copy(t).start()

        for b in order:
            prod[b] = lax.dot_general(
                gbuf[t], w[b], (((1,), (1,)), ((), ())), preferred_element_type=jnp.float32
            )
            if b >= 1:
                @pl.when(j == 0)
                def _():
                    rs_s[t, 0, n - 1 - b] = prod[b].astype(jnp.bfloat16)
                    rs_copy(t, 0, n - 1 - b).start()
            if b <= n - 2:
                @pl.when(j == n - 1)
                def _():
                    rs_s[t, 1, b] = prod[b].astype(jnp.bfloat16)
                    rs_copy(t, 1, b).start()

        def take(block):
            value = xg[t, block]
            acc[...] += jnp.dot(value, w[block], preferred_element_type=jnp.float32)
            value_wide = value.astype(jnp.float32)
            ssq[...] += jnp.broadcast_to(rowsum(value_wide * value_wide), ssq.shape)

        acc[...] = jnp.zeros_like(acc)
        ssq[...] = jnp.zeros_like(ssq)
        take(j)

        for k in range(n - 1):
            for side in range(2):
                line_recv(*xs, t, side, k)
                line_send(*xs, t, side, k + 1)
            for side in range(2):
                if k > 0:
                    line_recv(*sts, t + 1, side, k - 1, more)
                line_send(*sts, t + 1, side, k, more)

            up, down = n - 1 - k, k

            @pl.when(both(j > 0, j < up))
            def _():
                rs_in(t, 0, k).wait_recv()
                rs_s[t, 0, k] = (prod[up] + rs_r[t, 0, k].astype(jnp.float32)).astype(jnp.bfloat16)
                rs_copy(t, 0, k).start()

            @pl.when(both(j < n - 1, j > down))
            def _():
                rs_in(t, 1, k).wait_recv()
                rs_s[t, 1, k] = (prod[down] + rs_r[t, 1, k].astype(jnp.float32)).astype(jnp.bfloat16)
                rs_copy(t, 1, k).start()

            for side in range(2):
                block = j - 1 - k if side == 0 else j + 1 + k
                pl.when(arrives(side, k))(lambda block=block: take(block))

        factor = lax.rsqrt(ssq[:, :1] / extent + EPSILON) * (1.0 / root)
        fwd[t] = (xg[t, j].astype(jnp.float32) + acc[...] * factor).astype(jnp.bfloat16)
        pl.when(both(more, s < sections - 1))(lambda: fwd_copy(t).start())

        @pl.when(j > 0)
        def _():
            rs_in(t, 0, n - 1 - j).wait_recv()
            prod[j] += rs_r[t, 0, n - 1 - j].astype(jnp.float32)

        @pl.when(j < n - 1)
        def _():
            rs_in(t, 1, j).wait_recv()
            prod[j] += rs_r[t, 1, j].astype(jnp.float32)

        inner = inm[t]
        for q in range(1, n):
            inner_in(t, q).wait_recv()
            inner = inner + inb[t, q - 1]
        scale = ksc[:, :1]
        inner_dot = rowsum(inner) * scale * (1.0 / (root * extent))
        kept = st[t, j].astype(jnp.float32) * scale
        bwd[t] = (
            gbuf[t].astype(jnp.float32)
            + scale * (prod[j] * (1.0 / root) - kept * inner_dot)
        ).astype(jnp.bfloat16)
        pl.when(both(more, s > 0))(lambda: bwd_copy(t).start())

        for side in range(2):
            line_recv(*sts, t + 1, side, n - 2, more)
        pl.when(more)(lambda: stash_finish(t + 1))
        return carry

    lax.fori_loop(0, ticks, tick, 0)

    def drain(t, carry):
        for q in range(1, dp):
            for i in range(nb):
                dp_stash(t, q, i).wait_send()
                dp_stash_in(t, q, i).wait_recv()
            dp_grad(t, q).wait_send()
            dp_grad_in(t, q).wait_recv()
        for i in range(nb):
            own_stash(t, i).wait()
        own_grad_copy(t).wait()
        for q in range(1, n):
            inner_copy(t, q).wait_send()
        for k in range(n - 1):
            for side in range(2):
                line_sent(*xs, t, side, k)
                line_sent(*sts, t, side, k)
            pl.when(j < n - 1 - k)(lambda: rs_copy(t, 0, k).wait_send())
            pl.when(j > k)(lambda: rs_copy(t, 1, k).wait_send())
        pl.when(both(t < ticks - 1, s < sections - 1))(lambda: fwd_copy(t).wait_send())
        pl.when(both(t < ticks - 1, s > 0))(lambda: bwd_copy(t).wait_send())
        return carry

    lax.fori_loop(0, ticks, drain, 0)


def update_kernel(st, sg, m, wn, w_out, m_out):
    grads = lax.dot_general(
        st[0], sg[...], (((0,), (0,)), ((), ())), preferred_element_type=jnp.float32
    )
    velocity = MOMENTUM_RATE * m[...].astype(jnp.float32) + grads
    w_out[...] = (wn[...].astype(jnp.float32) - LEARNING_RATE * velocity).astype(jnp.bfloat16)
    m_out[...] = velocity.astype(jnp.bfloat16)


def body(
    n, dp, sections,
    shadow_weight_copy, newest_weight_version, momentum, pending_section_input,
    incoming_micro_input, pending_output_gradient, loss_gradient_rows, stashed,
):
    extent, cols = shadow_weight_copy.shape[1:]
    ticks, rows = stashed.shape[2:4]
    nb = n // dp
    bf16, f32 = jnp.bfloat16, jnp.float32
    dma = pltpu.SemaphoreType.DMA
    anywhere = pl.BlockSpec(memory_space=pl.ANY)
    vmem = pl.BlockSpec(memory_space=pltpu.VMEM)
    fwd, bwd, st_all, sg_all = pl.pallas_call(
        functools.partial(window_kernel, n, dp, sections),
        out_shape=(
            jax.ShapeDtypeStruct((ticks, rows, cols), bf16),
            jax.ShapeDtypeStruct((ticks, rows, cols), bf16),
            jax.ShapeDtypeStruct((nb, dp, ticks, rows, cols), bf16),
            jax.ShapeDtypeStruct((dp, ticks, rows, cols), bf16),
        ),
        in_specs=[anywhere] * 6,
        out_specs=(vmem, vmem, anywhere, anywhere),
        scratch_shapes=[
            pltpu.VMEM((n, cols, cols), bf16),
            pltpu.VMEM((ticks, n, rows, cols), bf16),
            pltpu.VMEM((ticks, n, rows, cols), bf16),
            pltpu.VMEM((ticks, rows, cols), bf16),
            pltpu.VMEM((n, rows, cols), f32),
            pltpu.VMEM((rows, cols), f32),
            pltpu.VMEM((rows, LANES), f32),
            pltpu.VMEM((rows, cols), f32),
            pltpu.VMEM((rows, LANES), f32),
            pltpu.VMEM((ticks, rows, cols), bf16),
            pltpu.VMEM((ticks, 2, n - 1, rows, cols), bf16),
            pltpu.VMEM((ticks, 2, n - 1, rows, cols), bf16),
            pltpu.VMEM((ticks, rows, LANES), f32),
            pltpu.VMEM((ticks, n - 1, rows, LANES), f32),
            dma((6,)),
            dma((ticks, 2, n - 1)),
            dma((ticks, 2, n - 1)),
            dma((ticks, 2, n - 1)),
            dma((ticks, 2, n - 1)),
            dma((ticks, 2, n - 1)),
            dma((ticks, 2, n - 1)),
            dma((ticks,)),
            dma((ticks,)),
            dma((ticks,)),
            dma((ticks,)),
            dma((ticks, n - 1)),
            dma((ticks, n - 1)),
            dma((ticks, dp - 1, nb)),
            dma((ticks, dp - 1, nb)),
            dma((ticks, dp - 1)),
            dma((ticks, dp - 1)),
            dma((ticks, nb + 1)),
        ],
        compiler_params=pltpu.CompilerParams(
            collective_id=0, has_side_effects=True, vmem_limit_bytes=48 * 1024 * 1024
        ),
        name="window",
    )(
        shadow_weight_copy.reshape(n, cols, cols),
        pending_section_input[0, 0],
        incoming_micro_input[0],
        pending_output_gradient[0, 0],
        loss_gradient_rows[0],
        stashed[0, 0],
    )
    depth = dp * ticks * rows
    own_rows = extent // dp
    tile = min(256, cols)
    per_block = cols // tile
    wide = pl.BlockSpec((tile, cols), lambda i: (i, 0))
    w_next, m_next = pl.pallas_call(
        update_kernel,
        out_shape=(jax.ShapeDtypeStruct((own_rows, cols), bf16),) * 2,
        grid=(own_rows // tile,),
        in_specs=[
            pl.BlockSpec((1, depth, tile), lambda i: (i // per_block, 0, i % per_block)),
            pl.BlockSpec((depth, cols), lambda i: (0, 0)),
            wide,
            wide,
        ],
        out_specs=(wide, wide),
        name="update",
    )(
        st_all.reshape(nb, depth, cols),
        sg_all.reshape(depth, cols),
        momentum[0],
        newest_weight_version[0],
    )
    return (fwd[None, None], bwd[None, None], w_next[None], m_next[None])


def solution(mesh):
    return jax.shard_map(
        functools.partial(body, mesh.shape["tensor"], mesh.shape["dp"], mesh.shape["section"]),
        mesh=mesh,
        in_specs=(
            P("section", None, "tensor"),
            P("section", "dp", "tensor"),
            P("section", "dp", "tensor"),
            P("dp", "section", None, "tensor"),
            P("dp", None, None, "tensor"),
            P("dp", "section", None, "tensor"),
            P("dp", None, None, "tensor"),
            P("dp", "section", None, None, "tensor"),
        ),
        out_specs=(
            P("dp", "section", None, None, "tensor"),
            P("dp", "section", None, None, "tensor"),
            P("section", "dp", "tensor"),
            P("section", "dp", "tensor"),
        ),
        check_vma=False,
    )
```

```python
import functools
import math

import jax
import jax.numpy as jnp
from jax import lax
from jax.experimental import pallas as pl
from jax.experimental.pallas import tpu as pltpu
from jax.sharding import PartitionSpec as P

EPSILON = 1e-06
MOMENTUM_RATE = 0.9
LEARNING_RATE = 0.05
MESH = pl.DeviceIdType.MESH
LANES = 128


def remote(src, dst, send_sem, recv_sem, target):
    return pltpu.make_async_remote_copy(
        src_ref=src,
        dst_ref=dst,
        send_sem=send_sem,
        recv_sem=recv_sem,
        device_id=target,
        device_id_type=MESH,
    )


def rowsum(values):
    return jnp.sum(values, axis=-1, keepdims=True)


def window_kernel(
    n, dp, sections,
    w_hbm, x0_hbm, inc_hbm, g0_hbm, loss_hbm, stash_hbm,
    fwd, bwd, st_all, sg_all,
    w, xg, st, gbuf, prod, acc, ssq, stw, ksc, sgs,
    rs_s, rs_r, inm, inb,
    lsem, x_ss, x_rs, st_ss, st_rs, rs_ss, rs_rs,
    f_ss, f_rs, b_ss, b_rs, in_ss, in_rs,
    dst_ss, dst_rs, dsg_ss, dsg_rs, own_sem,
):
    j = lax.axis_index("tensor")
    d = lax.axis_index("dp")
    s = lax.axis_index("section")
    ticks, _, rows, cols = xg.shape
    extent = n * cols
    root = math.sqrt(extent)
    nb = n // dp
    half = rows // 2
    halves = [pl.ds(h * half, half) for h in range(2)]
    first, last = s == 0, s == sections - 1

    def both(a, b):
        return jnp.logical_and(a, b)

    w_copy = pltpu.make_async_copy(w_hbm, w, lsem.at[0])
    st_copy = pltpu.make_async_copy(stash_hbm, st.at[:, j], lsem.at[1])
    x_copy = pltpu.make_async_copy(x0_hbm, xg.at[0, j], lsem.at[2])
    g_copy = pltpu.make_async_copy(g0_hbm, gbuf.at[0], lsem.at[3])
    inc_copy = pltpu.make_async_copy(inc_hbm, xg.at[pl.ds(1, ticks - 1), j], lsem.at[4])
    loss_copy = pltpu.make_async_copy(loss_hbm, gbuf.at[pl.ds(1, ticks - 1)], lsem.at[5])
    st_copy.start()
    x_copy.start()
    g_copy.start()
    pl.when(first)(lambda: inc_copy.start())
    pl.when(last)(lambda: loss_copy.start())
    w_copy.start()

    barrier = pltpu.get_barrier_semaphore()
    for q in range(1, n):
        pl.semaphore_signal(
            barrier, inc=1, device_id={"tensor": lax.rem(j + q, n)}, device_id_type=MESH
        )
    for q in range(1, dp):
        pl.semaphore_signal(
            barrier, inc=1, device_id={"dp": lax.rem(d + q, dp)}, device_id_type=MESH
        )

    @pl.when(s > 0)
    def _():
        pl.semaphore_signal(barrier, inc=1, device_id={"section": s - 1}, device_id_type=MESH)

    @pl.when(s < sections - 1)
    def _():
        pl.semaphore_signal(barrier, inc=1, device_id={"section": s + 1}, device_id_type=MESH)

    peers = n - 1 + dp - 1 + jnp.where(s > 0, 1, 0) + jnp.where(s < sections - 1, 1, 0)
    pl.semaphore_wait(barrier, peers)
    st_copy.wait()
    x_copy.wait()
    g_copy.wait()
    pl.when(first)(lambda: inc_copy.wait())
    pl.when(last)(lambda: loss_copy.wait())

    def line_copy(buf, ss, rs, t, side, k, h, block):
        piece = buf.at[t, block, halves[h]]
        return remote(
            piece, piece, ss.at[t, side, k, h], rs.at[t, side, k, h],
            {"tensor": j + 1 if side == 0 else j - 1},
        )

    def send_ok(side, k):
        if side == 0:
            return both(j < n - 1, j - k >= 0)
        return both(j > 0, j + k <= n - 1)

    def line_send(buf, ss, rs, t, side, k, h, extra=None):
        if k > n - 2:
            return
        ok = send_ok(side, k)
        ok = ok if extra is None else both(ok, extra)

        @pl.when(ok)
        def _():
            line_copy(buf, ss, rs, t, side, k, h, j - k if side == 0 else j + k).start()

    def line_sent(buf, ss, rs, t, side, k, h):
        @pl.when(send_ok(side, k))
        def _():
            line_copy(buf, ss, rs, t, side, k, h, j - k if side == 0 else j + k).wait_send()

    def arrives(side, k):
        return j - 1 - k >= 0 if side == 0 else j + 1 + k <= n - 1

    def line_recv(buf, ss, rs, t, side, k, h, extra=None):
        ok = arrives(side, k)
        ok = ok if extra is None else both(ok, extra)
        block = j - 1 - k if side == 0 else j + 1 + k

        @pl.when(ok)
        def _():
            piece = buf.at[t, block, halves[h]]
            remote(
                piece, piece, ss.at[t, side, k, h], rs.at[t, side, k, h],
                {"tensor": j - 1 if side == 0 else j + 1},
            ).wait_recv()

    xs = (xg, x_ss, x_rs)
    sts = (st, st_ss, st_rs)

    def dp_stash(t, q, i):
        peer = lax.rem(d + q, dp)
        return remote(
            st.at[t, peer * nb + i], st_all.at[i, d, t],
            dst_ss.at[t, q - 1, i], dst_rs.at[t, q - 1, i], {"dp": peer},
        )

    def dp_stash_in(t, q, i):
        peer = lax.rem(d + dp - q, dp)
        return remote(
            st.at[t, i], st_all.at[i, peer, t],
            dst_ss.at[t, q - 1, i], dst_rs.at[t, q - 1, i], {"dp": peer},
        )

    def dp_grad(t, q):
        peer = lax.rem(d + q, dp)
        return remote(
            sgs.at[t], sg_all.at[d, t], dsg_ss.at[t, q - 1], dsg_rs.at[t, q - 1], {"dp": peer}
        )

    def dp_grad_in(t, q):
        peer = lax.rem(d + dp - q, dp)
        return remote(
            sgs.at[t], sg_all.at[peer, t], dsg_ss.at[t, q - 1], dsg_rs.at[t, q - 1], {"dp": peer}
        )

    def own_stash(t, i):
        return pltpu.make_async_copy(st.at[t, d * nb + i], st_all.at[i, d, t], own_sem.at[t, i])

    def own_grad_copy(t):
        return pltpu.make_async_copy(sgs.at[t], sg_all.at[d, t], own_sem.at[t, nb])

    def stash_finish(t):
        for q in range(1, dp):
            for i in range(nb):
                dp_stash(t, q, i).start()
        for i in range(nb):
            own_stash(t, i).start()
        stw[...] = jnp.zeros_like(stw)

        def one(b, total):
            block = st[t, b]
            stw[...] += jnp.dot(block, w[b], preferred_element_type=jnp.float32)
            wide = block.astype(jnp.float32)
            return total + rowsum(wide * wide)

        total = lax.fori_loop(0, n, one, jnp.zeros((rows, 1), jnp.float32))
        ksc[...] = jnp.broadcast_to(lax.rsqrt(total / extent + EPSILON), ksc.shape)

    def rs_copy(t, side, k, h):
        return remote(
            rs_s.at[t, side, k, halves[h]], rs_r.at[t, side, k, halves[h]],
            rs_ss.at[t, side, k, h], rs_rs.at[t, side, k, h],
            {"tensor": j + 1 if side == 0 else j - 1},
        )

    def rs_in(t, side, k, h):
        return remote(
            rs_s.at[t, side, 0, halves[h]], rs_r.at[t, side, k, halves[h]],
            rs_ss.at[t, side, 0, h], rs_rs.at[t, side, k, h],
            {"tensor": j - 1 if side == 0 else j + 1},
        )

    def inner_copy(t, q):
        return remote(
            inm.at[t], inb.at[t, q - 1], in_ss.at[t, q - 1], in_rs.at[t, q - 1],
            {"tensor": lax.rem(j + q, n)},
        )

    def inner_in(t, q):
        return remote(
            inm.at[t], inb.at[t, q - 1], in_ss.at[t, q - 1], in_rs.at[t, q - 1],
            {"tensor": lax.rem(j + n - q, n)},
        )

    def fwd_copy(t):
        return remote(
            fwd.at[t], xg.at[t + 1, j], f_ss.at[t + 1], f_rs.at[t + 1], {"section": s + 1}
        )

    def bwd_copy(t):
        return remote(
            bwd.at[t], gbuf.at[t + 1], b_ss.at[t + 1], b_rs.at[t + 1], {"section": s - 1}
        )

    order = []
    for k in range((n + 1) // 2):
        order += [n - 1 - k] + ([k] if k != n - 1 - k else [])

    for h in range(2):
        for side in range(2):
            line_send(*sts, 0, side, 0, h)
    for k in range(n - 1):
        for h in range(2):
            for side in range(2):
                line_recv(*sts, 0, side, k, h)
                line_send(*sts, 0, side, k + 1, h)
    w_copy.wait()
    stash_finish(0)

    def tick(t, carry):
        more = t < ticks - 1

        @pl.when(both(t > 0, s > 0))
        def _():
            remote(
                fwd.at[t], xg.at[t, j], f_ss.at[t], f_rs.at[t], {"section": s - 1}
            ).wait_recv()

        for h in range(2):
            for side in range(2):
                line_send(*xs, t, side, 0, h)

        @pl.when(both(t > 0, s < sections - 1))
        def _():
            remote(
                bwd.at[t], gbuf.at[t], b_ss.at[t], b_rs.at[t], {"section": s + 1}
            ).wait_recv()

        wide = gbuf[t].astype(jnp.float32)
        products = wide * stw[...]
        part = products[:, :LANES]
        for i in range(1, cols // LANES):
            part = part + products[:, i * LANES:(i + 1) * LANES]
        inm[t] = part
        sgs[t] = (wide * (ksc[:, :1] * (1.0 / root))).astype(jnp.bfloat16)
        for q in range(1, n):
            inner_copy(t, q).start()
        for q in range(1, dp):
            dp_grad(t, q).start()
        own_grad_copy(t).start()

        for b in order:
            prod[b] = lax.dot_general(
                gbuf[t], w[b], (((1,), (1,)), ((), ())), preferred_element_type=jnp.float32
            )
            if b >= 1:
                @pl.when(j == 0)
                def _():
                    rs_s[t, 0, n - 1 - b] = prod[b].astype(jnp.bfloat16)
                    for h in range(2):
                        rs_copy(t, 0, n - 1 - b, h).start()
            if b <= n - 2:
                @pl.when(j == n - 1)
                def _():
                    rs_s[t, 1, b] = prod[b].astype(jnp.bfloat16)
                    for h in range(2):
                        rs_copy(t, 1, b, h).start()

        def take(block):
            value = xg[t, block]
            acc[...] += jnp.dot(value, w[block], preferred_element_type=jnp.float32)
            value_wide = value.astype(jnp.float32)
            ssq[...] += jnp.broadcast_to(rowsum(value_wide * value_wide), ssq.shape)

        acc[...] = jnp.zeros_like(acc)
        ssq[...] = jnp.zeros_like(ssq)
        take(j)

        for k in range(n - 1):
            for h in range(2):
                for side in range(2):
                    line_recv(*xs, t, side, k, h)
                    line_send(*xs, t, side, k + 1, h)

            up, down = n - 1 - k, k

            @pl.when(both(j > 0, j < up))
            def _():
                for h in range(2):
                    at = halves[h]
                    rs_in(t, 0, k, h).wait_recv()
                    total = prod[up, at] + rs_r[t, 0, k, at].astype(jnp.float32)
                    rs_s[t, 0, k, at] = total.astype(jnp.bfloat16)
                    rs_copy(t, 0, k, h).start()

            @pl.when(both(j < n - 1, j > down))
            def _():
                for h in range(2):
                    at = halves[h]
                    rs_in(t, 1, k, h).wait_recv()
                    total = prod[down, at] + rs_r[t, 1, k, at].astype(jnp.float32)
                    rs_s[t, 1, k, at] = total.astype(jnp.bfloat16)
                    rs_copy(t, 1, k, h).start()

            for side in range(2):
                block = j - 1 - k if side == 0 else j + 1 + k
                pl.when(arrives(side, k))(lambda block=block: take(block))
            for h in range(2):
                for side in range(2):
                    if k > 0:
                        line_recv(*sts, t + 1, side, k - 1, h, more)
                    line_send(*sts, t + 1, side, k, h, more)

        factor = lax.rsqrt(ssq[:, :1] / extent + EPSILON) * (1.0 / root)
        fwd[t] = (xg[t, j].astype(jnp.float32) + acc[...] * factor).astype(jnp.bfloat16)
        pl.when(both(more, s < sections - 1))(lambda: fwd_copy(t).start())

        @pl.when(j > 0)
        def _():
            for h in range(2):
                rs_in(t, 0, n - 1 - j, h).wait_recv()
            prod[j] += rs_r[t, 0, n - 1 - j].astype(jnp.float32)

        @pl.when(j < n - 1)
        def _():
            for h in range(2):
                rs_in(t, 1, j, h).wait_recv()
            prod[j] += rs_r[t, 1, j].astype(jnp.float32)

        inner = inm[t]
        for q in range(1, n):
            inner_in(t, q).wait_recv()
            inner = inner + inb[t, q - 1]
        scale = ksc[:, :1]
        inner_dot = rowsum(inner) * scale * (1.0 / (root * extent))
        kept = st[t, j].astype(jnp.float32) * scale
        bwd[t] = (
            gbuf[t].astype(jnp.float32)
            + scale * (prod[j] * (1.0 / root) - kept * inner_dot)
        ).astype(jnp.bfloat16)
        pl.when(both(more, s > 0))(lambda: bwd_copy(t).start())

        for h in range(2):
            for side in range(2):
                line_recv(*sts, t + 1, side, n - 2, h, more)
        pl.when(more)(lambda: stash_finish(t + 1))
        return carry

    lax.fori_loop(0, ticks, tick, 0)

    def drain(t, carry):
        for q in range(1, dp):
            for i in range(nb):
                dp_stash(t, q, i).wait_send()
                dp_stash_in(t, q, i).wait_recv()
            dp_grad(t, q).wait_send()
            dp_grad_in(t, q).wait_recv()
        for i in range(nb):
            own_stash(t, i).wait()
        own_grad_copy(t).wait()
        for q in range(1, n):
            inner_copy(t, q).wait_send()
        for k in range(n - 1):
            for h in range(2):
                for side in range(2):
                    line_sent(*xs, t, side, k, h)
                    line_sent(*sts, t, side, k, h)
                pl.when(j < n - 1 - k)(lambda: rs_copy(t, 0, k, h).wait_send())
                pl.when(j > k)(lambda: rs_copy(t, 1, k, h).wait_send())
        pl.when(both(t < ticks - 1, s < sections - 1))(lambda: fwd_copy(t).wait_send())
        pl.when(both(t < ticks - 1, s > 0))(lambda: bwd_copy(t).wait_send())
        return carry

    lax.fori_loop(0, ticks, drain, 0)


def update_kernel(st, sg, m, wn, w_out, m_out):
    grads = lax.dot_general(
        st[0], sg[...], (((0,), (0,)), ((), ())), preferred_element_type=jnp.float32
    )
    velocity = MOMENTUM_RATE * m[...].astype(jnp.float32) + grads
    w_out[...] = (wn[...].astype(jnp.float32) - LEARNING_RATE * velocity).astype(jnp.bfloat16)
    m_out[...] = velocity.astype(jnp.bfloat16)


def body(
    n, dp, sections,
    shadow_weight_copy, newest_weight_version, momentum, pending_section_input,
    incoming_micro_input, pending_output_gradient, loss_gradient_rows, stashed,
):
    extent, cols = shadow_weight_copy.shape[1:]
    ticks, rows = stashed.shape[2:4]
    nb = n // dp
    bf16, f32 = jnp.bfloat16, jnp.float32
    dma = pltpu.SemaphoreType.DMA
    anywhere = pl.BlockSpec(memory_space=pl.ANY)
    vmem = pl.BlockSpec(memory_space=pltpu.VMEM)
    fwd, bwd, st_all, sg_all = pl.pallas_call(
        functools.partial(window_kernel, n, dp, sections),
        out_shape=(
            jax.ShapeDtypeStruct((ticks, rows, cols), bf16),
            jax.ShapeDtypeStruct((ticks, rows, cols), bf16),
            jax.ShapeDtypeStruct((nb, dp, ticks, rows, cols), bf16),
            jax.ShapeDtypeStruct((dp, ticks, rows, cols), bf16),
        ),
        in_specs=[anywhere] * 6,
        out_specs=(vmem, vmem, anywhere, anywhere),
        scratch_shapes=[
            pltpu.VMEM((n, cols, cols), bf16),
            pltpu.VMEM((ticks, n, rows, cols), bf16),
            pltpu.VMEM((ticks, n, rows, cols), bf16),
            pltpu.VMEM((ticks, rows, cols), bf16),
            pltpu.VMEM((n, rows, cols), f32),
            pltpu.VMEM((rows, cols), f32),
            pltpu.VMEM((rows, LANES), f32),
            pltpu.VMEM((rows, cols), f32),
            pltpu.VMEM((rows, LANES), f32),
            pltpu.VMEM((ticks, rows, cols), bf16),
            pltpu.VMEM((ticks, 2, n - 1, rows, cols), bf16),
            pltpu.VMEM((ticks, 2, n - 1, rows, cols), bf16),
            pltpu.VMEM((ticks, rows, LANES), f32),
            pltpu.VMEM((ticks, n - 1, rows, LANES), f32),
            dma((6,)),
            dma((ticks, 2, n - 1, 2)),
            dma((ticks, 2, n - 1, 2)),
            dma((ticks, 2, n - 1, 2)),
            dma((ticks, 2, n - 1, 2)),
            dma((ticks, 2, n - 1, 2)),
            dma((ticks, 2, n - 1, 2)),
            dma((ticks,)),
            dma((ticks,)),
            dma((ticks,)),
            dma((ticks,)),
            dma((ticks, n - 1)),
            dma((ticks, n - 1)),
            dma((ticks, dp - 1, nb)),
            dma((ticks, dp - 1, nb)),
            dma((ticks, dp - 1)),
            dma((ticks, dp - 1)),
            dma((ticks, nb + 1)),
        ],
        compiler_params=pltpu.CompilerParams(
            collective_id=0, has_side_effects=True, vmem_limit_bytes=48 * 1024 * 1024
        ),
        name="window",
    )(
        shadow_weight_copy.reshape(n, cols, cols),
        pending_section_input[0, 0],
        incoming_micro_input[0],
        pending_output_gradient[0, 0],
        loss_gradient_rows[0],
        stashed[0, 0],
    )
    depth = dp * ticks * rows
    own_rows = extent // dp
    tile = min(256, cols)
    per_block = cols // tile
    wide = pl.BlockSpec((tile, cols), lambda i: (i, 0))
    w_next, m_next = pl.pallas_call(
        update_kernel,
        out_shape=(jax.ShapeDtypeStruct((own_rows, cols), bf16),) * 2,
        grid=(own_rows // tile,),
        in_specs=[
            pl.BlockSpec((1, depth, tile), lambda i: (i // per_block, 0, i % per_block)),
            pl.BlockSpec((depth, cols), lambda i: (0, 0)),
            wide,
            wide,
        ],
        out_specs=(wide, wide),
        name="update",
    )(
        st_all.reshape(nb, depth, cols),
        sg_all.reshape(depth, cols),
        momentum[0],
        newest_weight_version[0],
    )
    return (fwd[None, None], bwd[None, None], w_next[None], m_next[None])


def solution(mesh):
    return jax.shard_map(
        functools.partial(body, mesh.shape["tensor"], mesh.shape["dp"], mesh.shape["section"]),
        mesh=mesh,
        in_specs=(
            P("section", None, "tensor"),
            P("section", "dp", "tensor"),
            P("section", "dp", "tensor"),
            P("dp", "section", None, "tensor"),
            P("dp", None, None, "tensor"),
            P("dp", "section", None, "tensor"),
            P("dp", None, None, "tensor"),
            P("dp", "section", None, None, "tensor"),
        ),
        out_specs=(
            P("dp", "section", None, None, "tensor"),
            P("dp", "section", None, None, "tensor"),
            P("section", "dp", "tensor"),
            P("section", "dp", "tensor"),
        ),
        check_vma=False,
    )
```
